32 devices in a mesh: fsdp: 8 (over z, y), tp: 4 (over x, core).
Axes of the slice: x: 2, y: 2, z: 4, core: 2. Of those that a mesh axis runs over, the one named last changes fastest.
Arguments:
- hidden_in: bfloat16 [1024, 8192], P('fsdp'), may hold values from -6 to 6
- key_grad: bfloat16 [1024, 1024], P('fsdp', 'tp'), may hold values from -2.5 to 2.5
- positions: int32 [1024], P('fsdp'), may hold values from 0 to 1023, as said below
- key_quant: bfloat16 [8704, 1024], P('fsdp', 'tp'), may hold values from -4 to 4
- key_scales: float32 [8704, 8], P('fsdp', 'tp'), may hold values from 0.01 to 0.1
- block_counts: int32 [8], replicated, may hold values from 960 to 1088, as said below
Outputs:
- weight_grad: bfloat16 [8704, 1024], P('fsdp', 'tp')
- input_grad: bfloat16 [1024, 8192], P('fsdp', 'tp')
The draws below stay inside these ranges and needn't reach their ends.
Inputs may be any that keep to these rules, and one draw needn't show every extreme that they name: Index f of fsdp owns the consecutive projection rows from block_counts[0] + ... + block_counts[f-1] on, in its first block_counts[f] slots; the counts sum to 8192, and some index owns exactly 1088 rows. positions count the tokens from the start of their packed document; the first token's document may have begun before the first token, and a document may go on into the next index's tokens.
All inputs are finite; a program needn't handle non-finite values.
Results may differ from the reference program's by a relative error of at most 0.013.
Values may be sent and summed in bfloat16 or wider, within the bound.
A program may use at most 64 MiB of HBM per device.

```python
import math
import jax
import jax.numpy as jnp
from jax import lax

D = 8192
KVH = 8
HD = 128
TOKENS = 1024
SLOTS = 1088
N_FSDP = 8
N_TP = 4


def draw_block_counts(key, part):
    base_count = D // N_FSDP
    extra = SLOTS - base_count
    remain = D - N_FSDP * base_count
    order = jax.random.permutation(jax.random.fold_in(key, 11), N_FSDP)
    places = jnp.arange(N_FSDP, dtype=jnp.int32)
    values = base_count + (places < remain).astype(jnp.int32)
    pair_total = N_FSDP // 2
    amounts = jax.random.randint(jax.random.fold_in(key, 12), (pair_total,), 0, extra, dtype=jnp.int32)
    amounts = amounts.at[0].set(SLOTS - values[0])
    pair_idx = jnp.minimum(places // 2, pair_total - 1)
    signs = jnp.where(places % 2 == 0, 1, -1).astype(jnp.int32)
    moved = jnp.where(places // 2 < pair_total, signs * amounts[pair_idx], 0).astype(jnp.int32)
    values = values + moved
    return jnp.zeros((N_FSDP,), jnp.int32).at[order].set(values)


def draw_positions(key, part):
    token_ids = jnp.arange(TOKENS, dtype=jnp.int32)
    first_len = jax.random.randint(jax.random.fold_in(key, 22), (), TOKENS // 4, TOKENS // 2 + 1, dtype=jnp.int32)
    marks = jax.random.randint(jax.random.fold_in(key, 21), (TOKENS,), 0, 256, dtype=jnp.int32)
    opening = (marks == 0) & (token_ids >= first_len) | (token_ids == first_len)
    starts = jnp.where(opening, token_ids, 0).astype(jnp.int32)
    begins = lax.cummax(starts)
    later = (token_ids - begins).astype(jnp.int32)
    carried = (token_ids + TOKENS - first_len).astype(jnp.int32)
    return jnp.where(token_ids < first_len, carried, later).astype(jnp.int32)


def with_spikes(entries, own_key, source, target, parts, factor):
    def block_of(axis_at):
        return (jnp.arange(entries.shape[axis_at]) // (entries.shape[axis_at] // parts)).reshape((-1,) + (1,) * (entries.ndim - 1 - axis_at))

    near = jax.random.permutation(own_key, parts)[block_of(target)]
    other_side = (block_of(target) + parts // 2) % parts
    return jnp.where((block_of(source) == near) | (block_of(source) == other_side), factor * entries, entries)


def levels(own_key, shape, pieces, low, top_value):
    loudness, own = 1.0, jax.random.fold_in(own_key, 6)
    for position, shards_of in pieces:
        steps = jnp.exp(jax.random.uniform(jax.random.fold_in(own, position), (shards_of,), jnp.float32, low / len(pieces), top_value / len(pieces)))
        loudness = loudness * jnp.repeat(steps, shape[position] // shards_of).reshape([-1 if axis == position else 1 for axis in range(len(shape))])
    return loudness


def scatter_about(key, dims, deviation, most, shards=(), kind=jnp.bfloat16):
    gain = levels(key, dims, shards, -0.22, 0.18) if shards else 1.0
    result = jax.random.normal(key, dims, jnp.float32) * deviation * gain
    return jnp.minimum(jnp.maximum(result, -most), most).astype(kind)


def bell_draw_with(key, dims, scale, limit, cuts, heavy, kind=jnp.bfloat16):
    values = scale * jax.random.normal(key, dims, jnp.float32)
    if cuts:
        values = values * levels(key, dims, cuts, -0.22, 0.18)
    return jnp.clip(with_spikes(values, jax.random.fold_in(key, 3), *heavy), -limit, limit).astype(kind)


def setup_inputs(seed: int = 0) -> dict:
    splits = jax.random.split(jax.random.key(seed), 7)
    hidden_in = bell_draw_with(splits[0], (TOKENS, D), 1.0, 6.0, ((0, 8),), (0, 1, 8, 2.0))
    key_grad = scatter_about(splits[1], (TOKENS, KVH * HD), (TOKENS ** -0.25), 2.5, ((0, 8), (1, 4)))
    positions = draw_positions(jax.random.fold_in(splits[6], 71), 0)
    key_quant = scatter_about(splits[3], (N_FSDP * SLOTS, KVH * HD), 1.0, 4.0, ((0, 8), (1, 4)))
    key_scales = jnp.clip(jnp.exp(math.log(0.1) - 2.3025851 * jax.random.uniform(splits[4], (N_FSDP * SLOTS, KVH), jnp.float32) ** levels(splits[4], (N_FSDP * SLOTS, KVH), ((0, 8), (1, 4)), -0.2, 0.2)), 0.01, 0.1)
    block_counts = draw_block_counts(jax.random.fold_in(splits[6], 71), 0)
    return {"hidden_in": hidden_in, "key_grad": key_grad, "positions": positions, "key_quant": key_quant, "key_scales": key_scales, "block_counts": block_counts}


rope_base = 500000.0


def rotary_backward(key_grad, positions):
    tokens_here = key_grad.shape[0]
    half_dim = HD // 2
    cotangent = key_grad.astype(jnp.float32).reshape(tokens_here, -1, HD)
    freq_idx = jnp.arange(half_dim, dtype=jnp.float32)
    inverse = jnp.exp(-(2.0 * freq_idx / HD) * math.log(rope_base))
    angles = positions.astype(jnp.float32)[:, None] * inverse[None, :]
    cosine = jnp.cos(angles)[:, None, :]
    sine_part = jnp.sin(angles)[:, None, :]
    lower_half = cotangent[..., :half_dim]
    upper_half = cotangent[..., half_dim:]
    back_lower = lower_half * cosine + upper_half * sine_part
    back_upper = upper_half * cosine - lower_half * sine_part
    joined = jnp.concatenate([back_lower, back_upper], axis=-1)
    return joined.reshape(tokens_here, -1).astype(jnp.bfloat16)


def slot_tables(block_counts, slot_count, row_total):
    counts = block_counts.astype(jnp.int32)
    offsets = (jnp.cumsum(counts) - counts).astype(jnp.int32)
    owners_n = counts.shape[0]
    slot_ids = jnp.arange(owners_n * slot_count, dtype=jnp.int32)
    within = slot_ids % slot_count
    live_counts = jnp.broadcast_to(counts[:, None], (owners_n, slot_count)).reshape(-1)
    base_rows = jnp.broadcast_to(offsets[:, None], (owners_n, slot_count)).reshape(-1)
    is_live = within < live_counts
    row_of_slot = jnp.where(is_live, base_rows + within, 0).astype(jnp.int32)
    row_ids = jnp.arange(row_total, dtype=jnp.int32)
    at_or_after = row_ids[:, None] >= offsets[None, :]
    owner_of_row = jnp.sum(at_or_after.astype(jnp.int32), axis=1) - 1
    row_begin = jnp.max(jnp.where(at_or_after, offsets[None, :], 0), axis=1)
    slot_of_row = (owner_of_row * slot_count + row_ids - row_begin).astype(jnp.int32)
    return row_of_slot, is_live, slot_of_row


def reference(hidden_in, key_grad, positions, key_quant, key_scales, block_counts):
    row_of_slot, is_live, slot_of_row = slot_tables(block_counts, SLOTS, D)
    scaled = key_quant.astype(jnp.float32).reshape(-1, KVH, HD) * key_scales[:, :, None]
    weights_slots = scaled.astype(jnp.bfloat16).reshape(-1, KVH * HD)
    weights = jnp.take(weights_slots, slot_of_row, axis=0)
    rotated = rotary_backward(key_grad, positions)
    grad_full = jnp.dot(hidden_in.T, rotated, preferred_element_type=jnp.float32)
    grad_slots = jnp.where(is_live[:, None], jnp.take(grad_full, row_of_slot, axis=0), jnp.zeros((), jnp.float32))
    group_width = KVH * HD // N_TP
    total = jnp.zeros((rotated.shape[0], D), jnp.float32)
    for group in range(N_TP):
        lo_col = group * group_width
        part_rot = rotated[:, lo_col:lo_col + group_width]
        part_w = weights[:, lo_col:lo_col + group_width]
        group_part = jnp.dot(part_rot, part_w.T, preferred_element_type=jnp.float32).astype(jnp.bfloat16)
        total = total + group_part.astype(jnp.float32)
    return grad_slots.astype(jnp.bfloat16), total.astype(jnp.bfloat16)
```

```python
import functools
import math

import jax
import jax.numpy as jnp
from jax import lax
from jax.experimental import pallas as pl
from jax.experimental.pallas import tpu as pltpu
from jax.sharding import PartitionSpec as P

HD = 128
LANES = 128
LINE = 2
MESH = pl.DeviceIdType.MESH

rope_base = 500000.0


def rotary_tables(positions):
    half_dim = HD // 2
    freq_idx = jnp.arange(half_dim, dtype=jnp.float32)
    inverse = jnp.exp(-(2.0 * freq_idx / HD) * math.log(rope_base))
    angles = positions.astype(jnp.float32)[:, None] * inverse[None, :]
    return jnp.cos(angles), jnp.sin(angles)


def offset_range(index, owners_n, row_total, slot_count):
    least_count = 2 * row_total // owners_n - slot_count
    later = owners_n - index
    least = max(index * least_count, row_total - later * slot_count)
    greatest = min(index * slot_count, row_total - later * least_count)
    return least, greatest


def exchange_fits(owners_n, group_total, slot_count, row_total, tokens_here, width):
    if group_total % 2 or owners_n % group_total or owners_n % LINE or slot_count % (16 * group_total):
        return False
    if tokens_here % LANES or width % LANES or row_total % group_total or (row_total // group_total) % LANES:
        return False
    quarter = slot_count // group_total
    chunk = row_total // group_total
    per_chunk = owners_n // group_total
    if 2 * row_total // owners_n - slot_count < quarter or row_total < 2 * quarter + 4 * LANES:
        return False
    for owner in range(owners_n):
        least, greatest = offset_range(owner, owners_n, row_total, slot_count)
        home = owner // per_chunk
        for part in range(group_total):
            reach = range(
                max(0, (least + part * quarter) // chunk),
                min(group_total - 1, (greatest + (part + 1) * quarter - 1) // chunk) + 1,
            )
            allowed = {home}
            if part == 0 and owner % per_chunk == 0:
                allowed.add(home - 1)
            if part == group_total - 1 and owner % per_chunk == per_chunk - 1:
                allowed.add(home + 1)
            if not set(reach) <= allowed:
                return False
    return True


def prepare_kernel(
    owners_n, group_total, span, counts_ref, hidden_ref, grad_ref, cos_ref, sin_ref, quant_ref, scales_ref,
    rot_ref, weights_ref, picked_ref, shifted
):
    part = lax.axis_index("tp")
    row_total = hidden_ref.shape[1]
    quarter = picked_ref.shape[1]
    heads = scales_ref.shape[1]
    cosine = jnp.concatenate([cos_ref[...], cos_ref[...]], axis=1)
    sine = jnp.concatenate([sin_ref[...], -sin_ref[...]], axis=1)
    for head in range(heads):
        cols = pl.ds(head * HD, HD)
        values = grad_ref[:, cols].astype(jnp.float32)
        swapped = jnp.concatenate([values[:, HD // 2 :], values[:, : HD // 2]], axis=1)
        rot_ref[:, cols] = (values * cosine + swapped * sine).astype(jnp.bfloat16)
        scale = scales_ref[:, head : head + 1]
        weights_ref[:, cols] = (quant_ref[:, cols].astype(jnp.float32) * scale).astype(jnp.bfloat16)
    offset = jnp.int32(0)
    for owner in range(owners_n):
        count = counts_ref[owner]
        begin = jnp.minimum(offset + part * quarter, row_total)
        base = jnp.minimum((begin // LANES) * LANES, row_total - span)
        window = hidden_ref[:, pl.ds(pl.multiple_of(base, LANES), span)].astype(jnp.float32)
        buffer = shifted.at[owner % 2]
        buffer[pl.ds(0, span), :] = window.T
        moved = buffer[pl.ds(begin - base, quarter), :]
        slot = lax.broadcasted_iota(jnp.int32, moved.shape, 0) + part * quarter
        picked_ref[owner] = jnp.where(slot < count, moved, 0.0).astype(jnp.bfloat16)
        offset = offset + count


def assemble_kernel(owners_n, group_total, pad, counts_ref, pieces_ref, out_ref, rows):
    chunk_at = lax.axis_index("tp")
    chunk = out_ref.shape[1]
    quarter = pieces_ref.shape[1]
    per_chunk = owners_n // group_total
    offsets = []
    offset = jnp.int32(0)
    for owner in range(owners_n):
        offsets.append(offset)
        offset = offset + counts_ref[owner]

    def first_row(owner):
        found = jnp.int32(0)
        for candidate in range(owners_n):
            found = jnp.where(owner == candidate, offsets[candidate], found)
        return found

    limit = rows.shape[0] - quarter

    def place(index, begin):
        rows[pl.ds(jnp.clip(begin, 0, limit), quarter), :] = pieces_ref[index].astype(jnp.float32)

    origin = pad - chunk_at * chunk
    first = chunk_at * per_chunk
    below = first_row(first - 1) + (group_total - 1) * quarter + origin
    place(0, jnp.where(chunk_at > 0, below, 0))
    for near in range(per_chunk):
        start = first_row(first + near) + origin
        for part in range(group_total):
            place(1 + near * group_total + part, start + part * quarter)
    above = first_row(first + per_chunk) + origin
    last = 1 + per_chunk * group_total
    place(last, jnp.where(chunk_at < group_total - 1, above, limit))
    for at in range(0, chunk, LANES):
        out_ref[:, pl.ds(at, LANES)] = rows[pl.ds(pad + at, LANES), :].T.astype(jnp.bfloat16)


def exchange_kernel(
    owners_n, group_total, rot_ref, weights_ref, picked_ref, grad_out, pieces_out,
    rotated, weights, hidden, outgoing, grad_send,
    own_sem, tp_send, tp_recv, w_send, w_recv, h_send, h_recv,
    up_send, down_send, side_send, pair_send, net_recv, pair_recv,
    o_send, e_send, o_recv, g_send, g_recv, local_sem,
):
    here = lax.axis_index("fsdp")
    part = lax.axis_index("tp")
    core = lax.rem(part, 2)
    partner = part + 1 - 2 * core
    tokens, width = rot_ref.shape
    quarter = picked_ref.shape[1]
    half = width * group_total // 2
    depth = owners_n // LINE
    z = here // LINE
    y = lax.rem(here, LINE)
    beside = z * LINE + (1 - y)
    per_chunk = owners_n // group_total
    home = here // per_chunk
    last_piece = 1 + per_chunk * group_total

    def remote(src, dst, send, recv, where):
        return pltpu.make_async_remote_copy(
            src_ref=src, dst_ref=dst, send_sem=send, recv_sem=recv, device_id=where, device_id_type=MESH
        )

    def rows_of(owner):
        return pl.ds(pl.multiple_of(owner * tokens, tokens), tokens)

    def cols_of(group):
        return pl.ds(pl.multiple_of(group * width, width), width)

    def slots_of(group):
        return pl.ds(pl.multiple_of(group * quarter, 16), quarter)

    def spread(step):
        target = lax.rem(part + step, group_total)
        block = rotated.at[rows_of(here), cols_of(part)]
        return remote(rot_ref, block, tp_send.at[step - 1], tp_recv.at[step - 1], (here, target))

    def weigh(step):
        target = lax.rem(part + step, group_total)
        return remote(
            weights_ref.at[slots_of(target), :], weights.at[:, cols_of(part)],
            w_send.at[step - 1], w_recv.at[step - 1], (here, target),
        )

    def hide(step):
        target = lax.rem(here + step, owners_n)
        return remote(
            picked_ref.at[target], hidden.at[:, rows_of(here)],
            h_send.at[step - 1], h_recv.at[step - 1], (target, part),
        )

    def relay(owner, send, where):
        view = rotated.at[rows_of(owner), pl.ds(pl.multiple_of(core * half, half), half)]
        return remote(view, view, send.at[owner], net_recv.at[owner], (where, part))

    def share(owner):
        view = rotated.at[rows_of(owner), pl.ds(pl.multiple_of(core * half, half), half)]
        return remote(view, view, pair_send.at[owner], pair_recv.at[owner], (here, partner))

    own_rot = pltpu.make_async_copy(rot_ref, rotated.at[rows_of(here), cols_of(part)], own_sem.at[0])
    own_weights = pltpu.make_async_copy(
        weights_ref.at[slots_of(part), :], weights.at[:, cols_of(part)], own_sem.at[1]
    )
    own_hidden = pltpu.make_async_copy(picked_ref.at[here], hidden.at[:, rows_of(here)], own_sem.at[2])
    own_rot.start()
    own_weights.start()
    own_hidden.start()
    for step in range(1, group_total):
        spread(step).start()
    for step in range(1, group_total):
        weigh(step).start()
    own_rot.wait()
    for step in range(1, group_total):
        spread(step).wait_recv()

    below, above = here - LINE, here + LINE

    def travel(owner, go_up, go_down, act):
        @pl.when(go_up)
        def _():
            act(relay(owner, up_send, above))

        @pl.when(go_down)
        def _():
            act(relay(owner, down_send, below))

    def begin(copy):
        copy.start()

    def finish(copy):
        copy.wait_send()

    travel(here, z < depth - 1, z > 0, begin)
    relay(here, side_send, beside).start()
    for away in range(1, depth + 1):
        for sign in (-1, 1):
            if away < depth:
                level = z + sign * away
                owner = level * LINE + y

                @pl.when((level >= 0) & (level < depth))
                def _():
                    relay(owner, up_send, here).wait_recv()
                    if sign < 0:
                        travel(owner, z < depth - 1, z < 0, begin)
                    else:
                        travel(owner, z < 0, z > 0, begin)
                    relay(owner, side_send, beside).start()
                    share(owner).start()

            if away > 1 or sign < 0:
                level_near = z + sign * (away - 1)
                other = level_near * LINE + (1 - y)

                @pl.when((level_near >= 0) & (level_near < depth))
                def _():
                    relay(other, up_send, here).wait_recv()
                    share(other).start()

    for step in range(1, owners_n):
        hide(step).start()

    own_weights.wait()
    for step in range(1, group_total):
        weigh(step).wait_recv()

    def send_piece(owner, act_remote, act_local):
        source = outgoing.at[owner]

        def give(to_chunk, index, send, slot):
            mine = (owner == here) & (to_chunk == part)

            @pl.when(jnp.logical_not(mine))
            def _():
                act_remote(remote(source, pieces_out.at[index], send, o_recv.at[index], (owner, to_chunk)))

            @pl.when(mine)
            def _():
                act_local(pltpu.make_async_copy(source, pieces_out.at[index], local_sem.at[slot]))

        near = lax.rem(here, per_chunk)
        give(home, 1 + near * group_total + part, o_send.at[owner], 0)

        @pl.when((near == per_chunk - 1) & (part == group_total - 1) & (home < group_total - 1))
        def _():
            give(home + 1, 0, e_send.at[owner], 1)

        @pl.when((near == 0) & (part == 0) & (home > 0))
        def _():
            give(home - 1, last_piece, e_send.at[owner], 1)

    def nothing(copy):
        pass

    def produce(step, carry):
        owner = lax.rem(here + step, owners_n)

        @pl.when(step > 0)
        def _():
            share(owner).wait_recv()

        outgoing[owner] = lax.dot_general(
            weights[...], rotated[rows_of(owner), :], (((1,), (1,)), ((), ())),
            preferred_element_type=jnp.float32,
        ).astype(jnp.bfloat16)

        @pl.when(step > 0)
        def _():
            send_piece(lax.rem(here + step - 1, owners_n), begin, begin)

        return carry

    lax.fori_loop(0, owners_n, produce, 0)
    send_piece(lax.rem(here + owners_n - 1, owners_n), begin, begin)

    own_hidden.wait()
    for step in range(1, owners_n):
        hide(step).wait_recv()

    def send_grad(step):
        target = lax.rem(part + step, group_total)
        return remote(
            grad_send.at[target], grad_out.at[part], g_send.at[step - 1], g_recv.at[step - 1], (here, target)
        )

    def reduce(step, carry):
        target = lax.rem(part + step, group_total)
        grad_send[target] = jnp.dot(
            hidden[...], rotated[:, cols_of(target)], preferred_element_type=jnp.float32
        ).astype(jnp.bfloat16)

        @pl.when(step > 1)
        def _():
            send_grad(step - 1).start()

        return carry

    lax.fori_loop(1, group_total + 1, reduce, 0)
    own_grad = pltpu.make_async_copy(grad_send.at[part], grad_out.at[part], own_sem.at[3])
    own_grad.start()

    for owner in range(owners_n):
        send_piece(jnp.int32(owner), finish, lambda copy: copy.wait())
    for near in range(per_chunk):
        for source in range(group_total):
            index = 1 + near * group_total + source

            @pl.when(jnp.logical_not((home == part) & (here == part * per_chunk + near) & (part == source)))
            def _():
                remote(outgoing.at[0], pieces_out.at[index], o_send.at[0], o_recv.at[index], (here, partner)).wait_recv()

    for index, exists, mine in (
        (0, part > 0, (here == part * per_chunk - 1) & (part == group_total - 1)),
        (last_piece, part < group_total - 1, (here == (part + 1) * per_chunk) & (part == 0)),
    ):

        @pl.when(exists & jnp.logical_not(mine))
        def _():
            remote(outgoing.at[0], pieces_out.at[index], o_send.at[0], o_recv.at[index], (here, partner)).wait_recv()

    own_grad.wait()
    for step in range(1, group_total):
        send_grad(step).wait_send()
        remote(grad_send.at[0], grad_out.at[0], g_send.at[step - 1], g_recv.at[step - 1], (here, partner)).wait_recv()
    for step in range(1, group_total):
        spread(step).wait_send()
        weigh(step).wait_send()
    for step in range(1, owners_n):
        hide(step).wait_send()
    travel(here, z < depth - 1, z > 0, finish)
    relay(here, side_send, beside).wait_send()
    for away in range(1, depth):
        for sign in (-1, 1):
            level = z + sign * away
            owner = level * LINE + y

            @pl.when((level >= 0) & (level < depth))
            def _():
                if sign < 0:
                    travel(owner, z < depth - 1, z < 0, finish)
                else:
                    travel(owner, z < 0, z > 0, finish)
                relay(owner, side_send, beside).wait_send()

    def drain(step, carry):
        share(lax.rem(here + step, owners_n)).wait_send()
        return carry

    lax.fori_loop(1, owners_n, drain, 0)


def exchange_plan(hidden_in, key_grad, positions, key_quant, key_scales, block_counts):
    owners_n = lax.axis_size("fsdp")
    group_total = lax.axis_size("tp")
    slot_count, width = key_quant.shape
    tokens_here, row_total = hidden_in.shape
    quarter = slot_count // group_total
    chunk = row_total // group_total
    per_chunk = owners_n // group_total
    columns = width * group_total
    vmem = pl.BlockSpec(memory_space=pltpu.VMEM)
    smem = pl.BlockSpec(memory_space=pltpu.SMEM)
    span = -(-(quarter + LANES) // LANES) * LANES
    cosine, sine = rotary_tables(positions)
    rot, local_weights, picked = pl.pallas_call(
        functools.partial(prepare_kernel, owners_n, group_total, span),
        out_shape=(
            jax.ShapeDtypeStruct((tokens_here, width), jnp.bfloat16),
            jax.ShapeDtypeStruct((slot_count, width), jnp.bfloat16),
            jax.ShapeDtypeStruct((owners_n, quarter, tokens_here), jnp.bfloat16),
        ),
        in_specs=[smem] + [vmem] * 6,
        out_specs=(vmem,) * 3,
        scratch_shapes=[pltpu.VMEM((2, 2 * span + quarter, tokens_here), jnp.float32)],
        name="prepare",
    )(block_counts, hidden_in, key_grad, cosine, sine, key_quant, key_scales)

    pieces_n = 2 + per_chunk * group_total
    dma = pltpu.SemaphoreType.DMA
    weight_grad, pieces = pl.pallas_call(
        functools.partial(exchange_kernel, owners_n, group_total),
        out_shape=(
            jax.ShapeDtypeStruct((group_total, quarter, width), jnp.bfloat16),
            jax.ShapeDtypeStruct((pieces_n, quarter, tokens_here), jnp.bfloat16),
        ),
        in_specs=[vmem] * 3,
        out_specs=(vmem,) * 2,
        scratch_shapes=[
            pltpu.VMEM((owners_n * tokens_here, columns), jnp.bfloat16),
            pltpu.VMEM((quarter, columns), jnp.bfloat16),
            pltpu.VMEM((quarter, owners_n * tokens_here), jnp.bfloat16),
            pltpu.VMEM((owners_n, quarter, tokens_here), jnp.bfloat16),
            pltpu.VMEM((group_total, quarter, width), jnp.bfloat16),
            dma((4,)),
            dma((group_total - 1,)), dma((group_total - 1,)),
            dma((group_total - 1,)), dma((group_total - 1,)),
            dma((owners_n - 1,)), dma((owners_n - 1,)),
            dma((owners_n,)), dma((owners_n,)), dma((owners_n,)), dma((owners_n,)),
            dma((owners_n,)), dma((owners_n,)),
            dma((owners_n,)), dma((owners_n,)), dma((pieces_n,)),
            dma((group_total - 1,)), dma((group_total - 1,)),
            dma((2,)),
        ],
        compiler_params=pltpu.CompilerParams(has_side_effects=True),
        name="exchange",
    )(rot, local_weights, picked)

    margin = max(
        max(
            chunk * (owner // per_chunk) - offset_range(owner - 1, owners_n, row_total, slot_count)[0]
            for owner in range(per_chunk, owners_n, per_chunk)
        ),
        2 * quarter,
    ) if group_total > 1 else 2 * quarter
    pad = -(-(margin + slot_count) // 8) * 8
    input_grad = pl.pallas_call(
        functools.partial(assemble_kernel, owners_n, group_total, pad),
        out_shape=jax.ShapeDtypeStruct((tokens_here, chunk), jnp.bfloat16),
        in_specs=[smem, vmem],
        out_specs=vmem,
        scratch_shapes=[pltpu.VMEM((chunk + 2 * pad, tokens_here), jnp.float32)],
        name="assemble",
    )(block_counts, pieces)
    return (weight_grad.reshape(slot_count, width), input_grad)


def rotary_backward(key_grad, positions):
    tokens_here = key_grad.shape[0]
    half_dim = HD // 2
    cotangent = key_grad.astype(jnp.float32).reshape(tokens_here, -1, HD)
    freq_idx = jnp.arange(half_dim, dtype=jnp.float32)
    inverse = jnp.exp(-(2.0 * freq_idx / HD) * math.log(rope_base))
    angles = positions.astype(jnp.float32)[:, None] * inverse[None, :]
    cosine = jnp.cos(angles)[:, None, :]
    sine_part = jnp.sin(angles)[:, None, :]
    lower_half = cotangent[..., :half_dim]
    upper_half = cotangent[..., half_dim:]
    back_lower = lower_half * cosine + upper_half * sine_part
    back_upper = upper_half * cosine - lower_half * sine_part
    joined = jnp.concatenate([back_lower, back_upper], axis=-1)
    return joined.reshape(tokens_here, -1).astype(jnp.bfloat16)


def slot_tables(block_counts, slot_count, row_total):
    offsets = jnp.cumsum(block_counts) - block_counts
    owners_n = block_counts.shape[0]
    slot_ids = jnp.arange(owners_n * slot_count, dtype=jnp.int32)
    within = slot_ids % slot_count
    live_counts = jnp.broadcast_to(block_counts[:, None], (owners_n, slot_count)).reshape(-1)
    base_rows = jnp.broadcast_to(offsets[:, None], (owners_n, slot_count)).reshape(-1)
    is_live = within < live_counts
    row_of_slot = jnp.where(is_live, base_rows + within, 0)
    row_ids = jnp.arange(row_total, dtype=jnp.int32)
    at_or_after = row_ids[:, None] >= offsets[None, :]
    owner_of_row = jnp.sum(at_or_after.astype(jnp.int32), axis=1) - 1
    row_begin = jnp.max(jnp.where(at_or_after, offsets[None, :], 0), axis=1)
    slot_of_row = owner_of_row * slot_count + row_ids - row_begin
    return (row_of_slot, is_live, slot_of_row)


def gather_plan(hidden_in, key_grad, positions, key_quant, key_scales, block_counts):
    slot_count = key_quant.shape[0]
    local_heads = key_scales.shape[1]
    row_total = hidden_in.shape[1]
    row_of_slot, is_live, slot_of_row = slot_tables(block_counts, slot_count, row_total)
    scaled = (
        key_quant.astype(jnp.float32).reshape(slot_count, local_heads, HD) * key_scales[:, :, None]
    )
    local_weights = scaled.astype(jnp.bfloat16).reshape(slot_count, local_heads * HD)
    rotated = rotary_backward(key_grad, positions)
    picked = jnp.where(
        is_live[None, :], jnp.take(hidden_in, row_of_slot, axis=1), jnp.zeros((), jnp.bfloat16)
    )
    weight_grad = lax.psum_scatter(
        lax.dot_general(
            picked, rotated, (((0,), (0,)), ((), ())), preferred_element_type=jnp.float32
        ),
        "fsdp",
        scatter_dimension=0,
        tiled=True,
    ).astype(jnp.bfloat16)
    group_total = lax.axis_size("tp")
    whole_slots = lax.all_gather(local_weights, "fsdp", axis=0, tiled=True)
    ordered = jnp.take(whole_slots, slot_of_row, axis=0)
    own_rows = lax.all_to_all(ordered, "tp", split_axis=0, concat_axis=1, tiled=True)
    all_heads = lax.all_gather(rotated, "tp", axis=1, tiled=True)
    tokens_here = all_heads.shape[0]
    feature_here = own_rows.shape[0]
    heads_grouped = all_heads.reshape(tokens_here, group_total, -1)
    rows_grouped = own_rows.reshape(feature_here, group_total, -1)
    group_part = jnp.einsum(
        "tgk,dgk->gtd", heads_grouped, rows_grouped, preferred_element_type=jnp.float32
    ).astype(jnp.bfloat16)
    input_grad = jnp.sum(group_part.astype(jnp.float32), axis=0).astype(jnp.bfloat16)
    return (weight_grad, input_grad)


def per_device(hidden_in, key_grad, positions, key_quant, key_scales, block_counts):
    tokens_here, row_total = hidden_in.shape
    slot_count, width = key_quant.shape
    fits = exchange_fits(
        lax.axis_size("fsdp"), lax.axis_size("tp"), slot_count, row_total, tokens_here, width
    )
    plan = exchange_plan if fits else gather_plan
    return plan(hidden_in, key_grad, positions, key_quant, key_scales, block_counts)


def solution(mesh):
    in_specs = (P("fsdp", None), P("fsdp", "tp"), P("fsdp"), P("fsdp", "tp"), P("fsdp", "tp"), P())
    out_specs = (P("fsdp", "tp"), P("fsdp", "tp"))
    return jax.shard_map(
        per_device, mesh=mesh, in_specs=in_specs, out_specs=out_specs, check_vma=False
    )
```

```python
import functools
import math

import jax
import jax.numpy as jnp
from jax import lax
from jax.experimental import pallas as pl
from jax.experimental.pallas import tpu as pltpu
from jax.sharding import PartitionSpec as P

HD = 128
LANES = 128
LINE = 2
MESH = pl.DeviceIdType.MESH

rope_base = 500000.0


def rotary_tables(positions):
    half_dim = HD // 2
    freq_idx = jnp.arange(half_dim, dtype=jnp.float32)
    inverse = jnp.exp(-(2.0 * freq_idx / HD) * math.log(rope_base))
    angles = positions.astype(jnp.float32)[:, None] * inverse[None, :]
    return jnp.cos(angles), jnp.sin(angles)


def offset_range(index, owners_n, row_total, slot_count):
    least_count = 2 * row_total // owners_n - slot_count
    later = owners_n - index
    least = max(index * least_count, row_total - later * slot_count)
    greatest = min(index * slot_count, row_total - later * least_count)
    return least, greatest


def exchange_fits(owners_n, group_total, slot_count, row_total, tokens_here, width):
    if group_total % 2 or owners_n % group_total or owners_n % LINE or slot_count % (16 * group_total):
        return False
    if tokens_here % LANES or width % LANES or row_total % group_total or (row_total // group_total) % LANES:
        return False
    quarter = slot_count // group_total
    chunk = row_total // group_total
    per_chunk = owners_n // group_total
    if 2 * row_total // owners_n - slot_count < quarter or row_total < 2 * quarter + 4 * LANES:
        return False
    for owner in range(owners_n):
        least, greatest = offset_range(owner, owners_n, row_total, slot_count)
        home = owner // per_chunk
        for part in range(group_total):
            reach = range(
                max(0, (least + part * quarter) // chunk),
                min(group_total - 1, (greatest + (part + 1) * quarter - 1) // chunk) + 1,
            )
            allowed = {home}
            if part == 0 and owner % per_chunk == 0:
                allowed.add(home - 1)
            if part == group_total - 1 and owner % per_chunk == per_chunk - 1:
                allowed.add(home + 1)
            if not set(reach) <= allowed:
                return False
    return True


def pick_kernel(owners_n, group_total, span, counts_ref, hidden_any, picked_ref, windows, shifted, load_sem):
    part = lax.axis_index("tp")
    row_total = hidden_any.shape[1]
    quarter = picked_ref.shape[1]
    offset = jnp.int32(0)
    plans = []
    for owner in range(owners_n):
        count = counts_ref[owner]
        start = jnp.minimum(offset + part * quarter, row_total)
        base = jnp.minimum((start // LANES) * LANES, row_total - span)
        load = pltpu.make_async_copy(
            hidden_any.at[:, pl.ds(pl.multiple_of(base, LANES), span)], windows.at[owner], load_sem.at[owner]
        )
        load.start()
        plans.append((count, start - base, load))
        offset = offset + count
    for owner, (count, shift, load) in enumerate(plans):
        load.wait()
        shifted[owner, pl.ds(0, span), :] = windows[owner].astype(jnp.float32).T
        moved = shifted[owner, pl.ds(shift, quarter), :]
        slot = lax.broadcasted_iota(jnp.int32, moved.shape, 0) + part * quarter
        picked_ref[owner] = jnp.where(slot < count, moved, 0.0).astype(jnp.bfloat16)


def assemble_kernel(owners_n, group_total, pad, counts_ref, pieces_ref, grad_ref, grad_out, out_ref, rows):
    chunk_at = lax.axis_index("tp")
    chunk = out_ref.shape[1]
    quarter = pieces_ref.shape[1]
    per_chunk = owners_n // group_total
    offsets = []
    offset = jnp.int32(0)
    for owner in range(owners_n):
        offsets.append(offset)
        offset = offset + counts_ref[owner]

    def first_row(owner):
        found = jnp.int32(0)
        for candidate in range(owners_n):
            found = jnp.where(owner == candidate, offsets[candidate], found)
        return found

    limit = rows.shape[0] - quarter

    def place(index, begin):
        rows[pl.ds(jnp.clip(begin, 0, limit), quarter), :] = pieces_ref[index].astype(jnp.float32)

    for part in range(group_total):
        grad_out[pl.ds(part * quarter, quarter), :] = grad_ref[part]
    origin = pad - chunk_at * chunk
    first = chunk_at * per_chunk
    below = first_row(first - 1) + (group_total - 1) * quarter + origin
    place(0, jnp.where(chunk_at > 0, below, 0))
    for near in range(per_chunk):
        start = first_row(first + near) + origin
        for part in range(group_total):
            place(1 + near * group_total + part, start + part * quarter)
    above = first_row(first + per_chunk) + origin
    last = 1 + per_chunk * group_total
    place(last, jnp.where(chunk_at < group_total - 1, above, limit))
    for at in range(0, chunk, LANES):
        out_ref[:, pl.ds(at, LANES)] = rows[pl.ds(pad + at, LANES), :].T.astype(jnp.bfloat16)


def exchange_kernel(
    owners_n, group_total, picked_ref, grad_ref, cos_ref, sin_ref, quant_ref, scales_ref,
    grad_out, pieces_out,
    rot_ref, weights_ref,
    rotated, weights, hidden, outgoing, grad_send,
    own_sem, tp_send, tp_recv, w_send, w_recv, h_send, h_recv,
    up_send, down_send, side_send, pair_send, net_recv, pair_recv,
    o_send, e_send, o_recv, g_send, g_recv, local_sem,
):
    here = lax.axis_index("fsdp")
    part = lax.axis_index("tp")
    core = lax.rem(part, 2)
    partner = part + 1 - 2 * core
    tokens, width = rot_ref.shape
    quarter = picked_ref.shape[1]
    half = width * group_total // 2
    depth = owners_n // LINE
    z = here // LINE
    y = lax.rem(here, LINE)
    beside = z * LINE + (1 - y)
    per_chunk = owners_n // group_total
    home = here // per_chunk
    last_piece = 1 + per_chunk * group_total

    def remote(src, dst, send, recv, where):
        return pltpu.make_async_remote_copy(
            src_ref=src, dst_ref=dst, send_sem=send, recv_sem=recv, device_id=where, device_id_type=MESH
        )

    def rows_of(owner):
        return pl.ds(pl.multiple_of(owner * tokens, tokens), tokens)

    def cols_of(group):
        return pl.ds(pl.multiple_of(group * width, width), width)

    def slots_of(group):
        return pl.ds(pl.multiple_of(group * quarter, 16), quarter)

    def spread(step):
        target = lax.rem(part + step, group_total)
        block = rotated.at[rows_of(here), cols_of(part)]
        return remote(rot_ref, block, tp_send.at[step - 1], tp_recv.at[step - 1], (here, target))

    def weigh(step):
        target = lax.rem(part + step, group_total)
        return remote(
            weights_ref.at[slots_of(target), :], weights.at[:, cols_of(part)],
            w_send.at[step - 1], w_recv.at[step - 1], (here, target),
        )

    def hide(target):
        return remote(
            picked_ref.at[target], hidden.at[:, rows_of(here)],
            h_send.at[target], h_recv.at[here], (target, part),
        )

    def hidden_from(owner):
        return remote(
            picked_ref.at[owner], hidden.at[:, rows_of(owner)],
            h_send.at[owner], h_recv.at[owner], (owner, part),
        )

    def relay(owner, send, where):
        view = rotated.at[rows_of(owner), pl.ds(pl.multiple_of(core * half, half), half)]
        return remote(view, view, send.at[owner], net_recv.at[owner], (where, part))

    def share(owner):
        view = rotated.at[rows_of(owner), pl.ds(pl.multiple_of(core * half, half), half)]
        return remote(view, view, pair_send.at[owner], pair_recv.at[owner], (here, partner))

    own_rot = pltpu.make_async_copy(rot_ref, rotated.at[rows_of(here), cols_of(part)], own_sem.at[0])
    own_weights = pltpu.make_async_copy(
        weights_ref.at[slots_of(part), :], weights.at[:, cols_of(part)], own_sem.at[1]
    )
    own_hidden = pltpu.make_async_copy(picked_ref.at[here], hidden.at[:, rows_of(here)], own_sem.at[2])
    own_hidden.start()
    heads = scales_ref.shape[0]
    cosine = jnp.concatenate([cos_ref[...], cos_ref[...]], axis=1)
    sine = jnp.concatenate([sin_ref[...], -sin_ref[...]], axis=1)
    for head in range(heads):
        cols = pl.ds(head * HD, HD)
        values = grad_ref[:, cols].astype(jnp.float32)
        swapped = jnp.concatenate([values[:, HD // 2 :], values[:, : HD // 2]], axis=1)
        rot_ref[:, cols] = (values * cosine + swapped * sine).astype(jnp.bfloat16)
    for head in range(heads):
        cols = pl.ds(head * HD, HD)
        scale = jnp.broadcast_to(scales_ref[head : head + 1, :], (HD, scales_ref.shape[1])).T
        weights_ref[:, cols] = (quant_ref[:, cols].astype(jnp.float32) * scale).astype(jnp.bfloat16)
        if head == 0:
            hide(beside).start()
            own_rot.start()
            for step in range(1, group_total):
                spread(step).start()
    own_weights.start()
    for step in range(1, group_total):
        weigh(step).start()

    def hide_at(rise, across):
        level = z + rise

        @pl.when((level >= 0) & (level < depth))
        def _():
            hide(level * LINE + (1 - y if across else y)).start()

    own_rot.wait()
    for step in range(1, group_total):
        spread(step).wait_recv()

    below, above = here - LINE, here + LINE

    def travel(owner, go_up, go_down, act):
        @pl.when(go_up)
        def _():
            act(relay(owner, up_send, above))

        @pl.when(go_down)
        def _():
            act(relay(owner, down_send, below))

    def begin(copy):
        copy.start()

    def finish(copy):
        copy.wait_send()

    def send_piece(owner, act_remote, act_local):
        source = outgoing.at[owner]

        def give(to_chunk, index, send, slot):
            mine = (owner == here) & (to_chunk == part)

            @pl.when(jnp.logical_not(mine))
            def _():
                act_remote(remote(source, pieces_out.at[index], send, o_recv.at[index], (owner, to_chunk)))

            @pl.when(mine)
            def _():
                act_local(pltpu.make_async_copy(source, pieces_out.at[index], local_sem.at[slot]))

        near = lax.rem(here, per_chunk)
        give(home, 1 + near * group_total + part, o_send.at[owner], 0)

        @pl.when((near == per_chunk - 1) & (part == group_total - 1) & (home < group_total - 1))
        def _():
            give(home + 1, 0, e_send.at[owner], 1)

        @pl.when((near == 0) & (part == 0) & (home > 0))
        def _():
            give(home - 1, last_piece, e_send.at[owner], 1)

    travel(here, z < depth - 1, z > 0, begin)
    relay(here, side_send, beside).start()
    hide_at(1, False)
    hide_at(-1, False)

    def produce(owner):
        outgoing[owner] = lax.dot_general(
            weights[...], rotated[rows_of(owner), :], (((1,), (1,)), ((), ())),
            preferred_element_type=jnp.float32,
        ).astype(jnp.bfloat16)

    own_weights.wait()
    for step in range(1, group_total):
        weigh(step).wait_recv()
    produce(here)

    def stage_items(away):
        items = []
        for sign in (-1, 1):
            if 0 < away < depth:
                items.append((z + sign * away, y))
            if away > 1 or (away == 1 and sign < 0):
                items.append((z + sign * (away - 1), 1 - y))
        return items

    send_piece(here, begin, begin)
    for away in range(1, depth + 2):
        for sign in (-1, 1):
            if away < depth:
                level = z + sign * away
                owner = level * LINE + y

                @pl.when((level >= 0) & (level < depth))
                def _():
                    relay(owner, up_send, here).wait_recv()
                    if sign < 0:
                        travel(owner, z < depth - 1, z < 0, begin)
                    else:
                        travel(owner, z < 0, z > 0, begin)
                    relay(owner, side_send, beside).start()
                    share(owner).start()

            if away <= depth and (away > 1 or sign < 0):
                level_near = z + sign * (away - 1)
                other = level_near * LINE + (1 - y)

                @pl.when((level_near >= 0) & (level_near < depth))
                def _():
                    relay(other, up_send, here).wait_recv()
                    share(other).start()

        if away < depth:
            hide_at(away, True)
            hide_at(-away, True)
        if away + 1 < depth:
            hide_at(away + 1, False)
            hide_at(-away - 1, False)
        ready = stage_items(away - 1)
        for level, row in ready:

            @pl.when((level >= 0) & (level < depth))
            def _():
                share(level * LINE + row).wait_recv()
                produce(level * LINE + row)

        for level, row in ready:

            @pl.when((level >= 0) & (level < depth))
            def _():
                send_piece(level * LINE + row, begin, begin)

    own_hidden.wait()
    for step in range(1, owners_n):
        hidden_from(lax.rem(here + step, owners_n)).wait_recv()

    def send_grad(step):
        target = lax.rem(part + step, group_total)
        return remote(
            grad_send.at[target], grad_out.at[part], g_send.at[step - 1], g_recv.at[step - 1], (here, target)
        )

    def reduce(step, carry):
        target = lax.rem(part + step, group_total)
        grad_send[target] = jnp.dot(
            hidden[...], rotated[:, cols_of(target)], preferred_element_type=jnp.float32
        ).astype(jnp.bfloat16)

        @pl.when(step > 1)
        def _():
            send_grad(step - 1).start()

        return carry

    lax.fori_loop(1, group_total + 1, reduce, 0)
    own_grad = pltpu.make_async_copy(grad_send.at[part], grad_out.at[part], own_sem.at[3])
    own_grad.start()

    for owner in range(owners_n):
        send_piece(jnp.int32(owner), finish, lambda copy: copy.wait())
    for near in range(per_chunk):
        for source in range(group_total):
            index = 1 + near * group_total + source

            @pl.when(jnp.logical_not((home == part) & (here == part * per_chunk + near) & (part == source)))
            def _():
                remote(outgoing.at[0], pieces_out.at[index], o_send.at[0], o_recv.at[index], (here, partner)).wait_recv()

    for index, exists, mine in (
        (0, part > 0, (here == part * per_chunk - 1) & (part == group_total - 1)),
        (last_piece, part < group_total - 1, (here == (part + 1) * per_chunk) & (part == 0)),
    ):

        @pl.when(exists & jnp.logical_not(mine))
        def _():
            remote(outgoing.at[0], pieces_out.at[index], o_send.at[0], o_recv.at[index], (here, partner)).wait_recv()

    own_grad.wait()
    for step in range(1, group_total):
        send_grad(step).wait_send()
        remote(grad_send.at[0], grad_out.at[0], g_send.at[step - 1], g_recv.at[step - 1], (here, partner)).wait_recv()
    for step in range(1, group_total):
        spread(step).wait_send()
        weigh(step).wait_send()
    for step in range(1, owners_n):
        hide(lax.rem(here + step, owners_n)).wait_send()
    travel(here, z < depth - 1, z > 0, finish)
    relay(here, side_send, beside).wait_send()
    for away in range(1, depth):
        for sign in (-1, 1):
            level = z + sign * away
            owner = level * LINE + y

            @pl.when((level >= 0) & (level < depth))
            def _():
                if sign < 0:
                    travel(owner, z < depth - 1, z < 0, finish)
                else:
                    travel(owner, z < 0, z > 0, finish)
                relay(owner, side_send, beside).wait_send()

    def drain(step, carry):
        share(lax.rem(here + step, owners_n)).wait_send()
        return carry

    lax.fori_loop(1, owners_n, drain, 0)


def exchange_plan(hidden_in, key_grad, positions, key_quant, key_scales, block_counts):
    owners_n = lax.axis_size("fsdp")
    group_total = lax.axis_size("tp")
    slot_count, width = key_quant.shape
    tokens_here, row_total = hidden_in.shape
    quarter = slot_count // group_total
    chunk = row_total // group_total
    per_chunk = owners_n // group_total
    columns = width * group_total
    vmem = pl.BlockSpec(memory_space=pltpu.VMEM)
    anywhere = pl.BlockSpec(memory_space=pl.ANY)
    smem = pl.BlockSpec(memory_space=pltpu.SMEM)
    span = -(-(quarter + LANES) // LANES) * LANES
    cosine, sine = rotary_tables(positions)
    picked = pl.pallas_call(
        functools.partial(pick_kernel, owners_n, group_total, span),
        out_shape=jax.ShapeDtypeStruct((owners_n, quarter, tokens_here), jnp.bfloat16),
        in_specs=[smem, anywhere],
        out_specs=vmem,
        scratch_shapes=[
            pltpu.VMEM((owners_n, tokens_here, span), jnp.bfloat16),
            pltpu.VMEM((owners_n, 2 * span + quarter, tokens_here), jnp.float32),
            pltpu.SemaphoreType.DMA((owners_n,)),
        ],
        name="pick",
    )(block_counts, hidden_in)

    pieces_n = 2 + per_chunk * group_total
    dma = pltpu.SemaphoreType.DMA
    weight_grad, pieces = pl.pallas_call(
        functools.partial(exchange_kernel, owners_n, group_total),
        out_shape=(
            jax.ShapeDtypeStruct((group_total, quarter, width), jnp.bfloat16),
            jax.ShapeDtypeStruct((pieces_n, quarter, tokens_here), jnp.bfloat16),
        ),
        in_specs=[vmem] * 6,
        out_specs=(vmem,) * 2,
        scratch_shapes=[
            pltpu.VMEM((tokens_here, width), jnp.bfloat16),
            pltpu.VMEM((slot_count, width), jnp.bfloat16),
            pltpu.VMEM((owners_n * tokens_here, columns), jnp.bfloat16),
            pltpu.VMEM((quarter, columns), jnp.bfloat16),
            pltpu.VMEM((quarter, owners_n * tokens_here), jnp.bfloat16),
            pltpu.VMEM((owners_n, quarter, tokens_here), jnp.bfloat16),
            pltpu.VMEM((group_total, quarter, width), jnp.bfloat16),
            dma((4,)),
            dma((group_total - 1,)), dma((group_total - 1,)),
            dma((group_total - 1,)), dma((group_total - 1,)),
            dma((owners_n,)), dma((owners_n,)),
            dma((owners_n,)), dma((owners_n,)), dma((owners_n,)), dma((owners_n,)),
            dma((owners_n,)), dma((owners_n,)),
            dma((owners_n,)), dma((owners_n,)), dma((pieces_n,)),
            dma((group_total - 1,)), dma((group_total - 1,)),
            dma((2,)),
        ],
        compiler_params=pltpu.CompilerParams(has_side_effects=True),
        name="exchange",
    )(picked, key_grad, cosine, sine, key_quant, key_scales.T)

    margin = max(
        max(
            chunk * (owner // per_chunk) - offset_range(owner - 1, owners_n, row_total, slot_count)[0]
            for owner in range(per_chunk, owners_n, per_chunk)
        ),
        2 * quarter,
    ) if group_total > 1 else 2 * quarter
    pad = -(-(margin + slot_count) // 8) * 8
    return pl.pallas_call(
        functools.partial(assemble_kernel, owners_n, group_total, pad),
        out_shape=(
            jax.ShapeDtypeStruct((slot_count, width), jnp.bfloat16),
            jax.ShapeDtypeStruct((tokens_here, chunk), jnp.bfloat16),
        ),
        in_specs=[smem, vmem, vmem],
        out_specs=(vmem,) * 2,
        scratch_shapes=[pltpu.VMEM((chunk + 2 * pad, tokens_here), jnp.float32)],
        name="assemble",
    )(block_counts, pieces, weight_grad)


def rotary_backward(key_grad, positions):
    tokens_here = key_grad.shape[0]
    half_dim = HD // 2
    cotangent = key_grad.astype(jnp.float32).reshape(tokens_here, -1, HD)
    freq_idx = jnp.arange(half_dim, dtype=jnp.float32)
    inverse = jnp.exp(-(2.0 * freq_idx / HD) * math.log(rope_base))
    angles = positions.astype(jnp.float32)[:, None] * inverse[None, :]
    cosine = jnp.cos(angles)[:, None, :]
    sine_part = jnp.sin(angles)[:, None, :]
    lower_half = cotangent[..., :half_dim]
    upper_half = cotangent[..., half_dim:]
    back_lower = lower_half * cosine + upper_half * sine_part
    back_upper = upper_half * cosine - lower_half * sine_part
    joined = jnp.concatenate([back_lower, back_upper], axis=-1)
    return joined.reshape(tokens_here, -1).astype(jnp.bfloat16)


def slot_tables(block_counts, slot_count, row_total):
    offsets = jnp.cumsum(block_counts) - block_counts
    owners_n = block_counts.shape[0]
    slot_ids = jnp.arange(owners_n * slot_count, dtype=jnp.int32)
    within = slot_ids % slot_count
    live_counts = jnp.broadcast_to(block_counts[:, None], (owners_n, slot_count)).reshape(-1)
    base_rows = jnp.broadcast_to(offsets[:, None], (owners_n, slot_count)).reshape(-1)
    is_live = within < live_counts
    row_of_slot = jnp.where(is_live, base_rows + within, 0)
    row_ids = jnp.arange(row_total, dtype=jnp.int32)
    at_or_after = row_ids[:, None] >= offsets[None, :]
    owner_of_row = jnp.sum(at_or_after.astype(jnp.int32), axis=1) - 1
    row_begin = jnp.max(jnp.where(at_or_after, offsets[None, :], 0), axis=1)
    slot_of_row = owner_of_row * slot_count + row_ids - row_begin
    return (row_of_slot, is_live, slot_of_row)


def gather_plan(hidden_in, key_grad, positions, key_quant, key_scales, block_counts):
    slot_count = key_quant.shape[0]
    local_heads = key_scales.shape[1]
    row_total = hidden_in.shape[1]
    row_of_slot, is_live, slot_of_row = slot_tables(block_counts, slot_count, row_total)
    scaled = (
        key_quant.astype(jnp.float32).reshape(slot_count, local_heads, HD) * key_scales[:, :, None]
    )
    local_weights = scaled.astype(jnp.bfloat16).reshape(slot_count, local_heads * HD)
    rotated = rotary_backward(key_grad, positions)
    picked = jnp.where(
        is_live[None, :], jnp.take(hidden_in, row_of_slot, axis=1), jnp.zeros((), jnp.bfloat16)
    )
    weight_grad = lax.psum_scatter(
        lax.dot_general(
            picked, rotated, (((0,), (0,)), ((), ())), preferred_element_type=jnp.float32
        ),
        "fsdp",
        scatter_dimension=0,
        tiled=True,
    ).astype(jnp.bfloat16)
    group_total = lax.axis_size("tp")
    whole_slots = lax.all_gather(local_weights, "fsdp", axis=0, tiled=True)
    ordered = jnp.take(whole_slots, slot_of_row, axis=0)
    own_rows = lax.all_to_all(ordered, "tp", split_axis=0, concat_axis=1, tiled=True)
    all_heads = lax.all_gather(rotated, "tp", axis=1, tiled=True)
    tokens_here = all_heads.shape[0]
    feature_here = own_rows.shape[0]
    heads_grouped = all_heads.reshape(tokens_here, group_total, -1)
    rows_grouped = own_rows.reshape(feature_here, group_total, -1)
    group_part = jnp.einsum(
        "tgk,dgk->gtd", heads_grouped, rows_grouped, preferred_element_type=jnp.float32
    ).astype(jnp.bfloat16)
    input_grad = jnp.sum(group_part.astype(jnp.float32), axis=0).astype(jnp.bfloat16)
    return (weight_grad, input_grad)


def per_device(hidden_in, key_grad, positions, key_quant, key_scales, block_counts):
    tokens_here, row_total = hidden_in.shape
    slot_count, width = key_quant.shape
    fits = exchange_fits(
        lax.axis_size("fsdp"), lax.axis_size("tp"), slot_count, row_total, tokens_here, width
    )
    plan = exchange_plan if fits else gather_plan
    return plan(hidden_in, key_grad, positions, key_quant, key_scales, block_counts)


def solution(mesh):
    in_specs = (P("fsdp", None), P("fsdp", "tp"), P("fsdp"), P("fsdp", "tp"), P("fsdp", "tp"), P())
    out_specs = (P("fsdp", "tp"), P("fsdp", "tp"))
    return jax.shard_map(
        per_device, mesh=mesh, in_specs=in_specs, out_specs=out_specs, check_vma=False
    )
```

```python
import functools
import math

import jax
import jax.numpy as jnp
from jax import lax
from jax.experimental import pallas as pl
from jax.experimental.pallas import tpu as pltpu
from jax.sharding import PartitionSpec as P

HD = 128
LANES = 128
LINE = 2
MESH = pl.DeviceIdType.MESH

rope_base = 500000.0


def rotary_tables(positions):
    half_dim = HD // 2
    freq_idx = jnp.arange(half_dim, dtype=jnp.float32)
    inverse = jnp.exp(-(2.0 * freq_idx / HD) * math.log(rope_base))
    angles = positions.astype(jnp.float32)[:, None] * inverse[None, :]
    return jnp.cos(angles), jnp.sin(angles)


def offset_range(index, owners_n, row_total, slot_count):
    least_count = 2 * row_total // owners_n - slot_count
    later = owners_n - index
    least = max(index * least_count, row_total - later * slot_count)
    greatest = min(index * slot_count, row_total - later * least_count)
    return least, greatest


def exchange_fits(owners_n, group_total, slot_count, row_total, tokens_here, width):
    if group_total % 2 or owners_n % group_total or owners_n % LINE or slot_count % (16 * group_total):
        return False
    if tokens_here % LANES or width % LANES or row_total % group_total or (row_total // group_total) % LANES:
        return False
    quarter = slot_count // group_total
    chunk = row_total // group_total
    per_chunk = owners_n // group_total
    if 2 * row_total // owners_n - slot_count < quarter or row_total < 2 * quarter + 4 * LANES:
        return False
    for owner in range(owners_n):
        least, greatest = offset_range(owner, owners_n, row_total, slot_count)
        home = owner // per_chunk
        for part in range(group_total):
            reach = range(
                max(0, (least + part * quarter) // chunk),
                min(group_total - 1, (greatest + (part + 1) * quarter - 1) // chunk) + 1,
            )
            allowed = {home}
            if part == 0 and owner % per_chunk == 0:
                allowed.add(home - 1)
            if part == group_total - 1 and owner % per_chunk == per_chunk - 1:
                allowed.add(home + 1)
            if not set(reach) <= allowed:
                return False
    return True


def pick_kernel(owners_n, group_total, span, counts_ref, hidden_any, picked_ref, windows, shifted, load_sem):
    part = lax.axis_index("tp")
    row_total = hidden_any.shape[1]
    quarter = picked_ref.shape[1]
    offset = jnp.int32(0)
    plans = []
    for owner in range(owners_n):
        count = counts_ref[owner]
        start = jnp.minimum(offset + part * quarter, row_total)
        base = jnp.minimum((start // LANES) * LANES, row_total - span)
        load = pltpu.make_async_copy(
            hidden_any.at[:, pl.ds(pl.multiple_of(base, LANES), span)], windows.at[owner], load_sem.at[owner]
        )
        load.start()
        plans.append((count, start - base, load))
        offset = offset + count
    for owner, (count, shift, load) in enumerate(plans):
        load.wait()
        shifted[owner, pl.ds(0, span), :] = windows[owner].astype(jnp.float32).T
        moved = shifted[owner, pl.ds(shift, quarter), :]
        slot = lax.broadcasted_iota(jnp.int32, moved.shape, 0) + part * quarter
        picked_ref[owner] = jnp.where(slot < count, moved, 0.0).astype(jnp.bfloat16)


def assemble_kernel(owners_n, group_total, pad, counts_ref, pieces_ref, grad_ref, grad_out, out_ref, rows):
    chunk_at = lax.axis_index("tp")
    chunk = out_ref.shape[1]
    quarter = pieces_ref.shape[1]
    per_chunk = owners_n // group_total
    offsets = []
    offset = jnp.int32(0)
    for owner in range(owners_n):
        offsets.append(offset)
        offset = offset + counts_ref[owner]

    def first_row(owner):
        found = jnp.int32(0)
        for candidate in range(owners_n):
            found = jnp.where(owner == candidate, offsets[candidate], found)
        return found

    limit = rows.shape[0] - quarter

    def place(index, begin):
        rows[pl.ds(jnp.clip(begin, 0, limit), quarter), :] = pieces_ref[index].astype(jnp.float32)

    for part in range(group_total):
        grad_out[pl.ds(part * quarter, quarter), :] = grad_ref[part]
    origin = pad - chunk_at * chunk
    first = chunk_at * per_chunk
    below = first_row(first - 1) + (group_total - 1) * quarter + origin
    place(0, jnp.where(chunk_at > 0, below, 0))
    for near in range(per_chunk):
        start = first_row(first + near) + origin
        for part in range(group_total):
            place(1 + near * group_total + part, start + part * quarter)
    above = first_row(first + per_chunk) + origin
    last = 1 + per_chunk * group_total
    place(last, jnp.where(chunk_at < group_total - 1, above, limit))
    for at in range(0, chunk, LANES):
        out_ref[:, pl.ds(at, LANES)] = rows[pl.ds(pad + at, LANES), :].T.astype(jnp.bfloat16)


def exchange_kernel(
    owners_n, group_total, picked_ref, grad_ref, cos_ref, sin_ref, quant_ref, scales_ref,
    grad_out, pieces_out,
    rot_ref, weights_ref,
    rotated, weights, hidden, outgoing, grad_send,
    own_sem, tp_send, tp_recv, w_send, w_recv, h_send, h_recv,
    up_send, down_send, side_send, pair_send, net_recv, pair_recv,
    o_send, e_send, o_recv, g_send, g_recv, local_sem,
):
    here = lax.axis_index("fsdp")
    part = lax.axis_index("tp")
    core = lax.rem(part, 2)
    partner = part + 1 - 2 * core
    tokens, width = rot_ref.shape
    quarter = picked_ref.shape[1]
    half = width * group_total // 2
    pieces = group_total // 2
    depth = owners_n // LINE
    z = here // LINE
    y = lax.rem(here, LINE)
    beside = z * LINE + (1 - y)
    per_chunk = owners_n // group_total
    home = here // per_chunk
    last_piece = 1 + per_chunk * group_total

    def remote(src, dst, send, recv, where):
        return pltpu.make_async_remote_copy(
            src_ref=src, dst_ref=dst, send_sem=send, recv_sem=recv, device_id=where, device_id_type=MESH
        )

    def rows_of(owner):
        return pl.ds(pl.multiple_of(owner * tokens, tokens), tokens)

    def cols_of(group):
        return pl.ds(pl.multiple_of(group * width, width), width)

    def slots_of(group):
        return pl.ds(pl.multiple_of(group * quarter, 16), quarter)

    def spread(step):
        target = lax.rem(part + step, group_total)
        block = rotated.at[rows_of(here), cols_of(part)]
        return remote(rot_ref, block, tp_send.at[step - 1], tp_recv.at[step - 1], (here, target))

    def weigh(step):
        target = lax.rem(part + step, group_total)
        return remote(
            weights_ref.at[slots_of(target), :], weights.at[:, cols_of(part)],
            w_send.at[step - 1], w_recv.at[step - 1], (here, target),
        )

    def hide(target):
        return remote(
            picked_ref.at[target], hidden.at[:, rows_of(here)],
            h_send.at[target], h_recv.at[here], (target, part),
        )

    def hidden_from(owner):
        return remote(
            picked_ref.at[owner], hidden.at[:, rows_of(owner)],
            h_send.at[owner], h_recv.at[owner], (owner, part),
        )

    def block_of(owner, piece):
        first = core * half + piece * width
        return rotated.at[rows_of(owner), pl.ds(pl.multiple_of(first, LANES), width)]

    def relay(owner, send, where, piece):
        view, at = block_of(owner, piece), owner * pieces + piece
        return remote(view, view, send.at[at], net_recv.at[at], (where, part))

    def share(owner, piece):
        view, at = block_of(owner, piece), owner * pieces + piece
        return remote(view, view, pair_send.at[at], pair_recv.at[at], (here, partner))

    own_rot = pltpu.make_async_copy(rot_ref, rotated.at[rows_of(here), cols_of(part)], own_sem.at[0])
    own_weights = pltpu.make_async_copy(
        weights_ref.at[slots_of(part), :], weights.at[:, cols_of(part)], own_sem.at[1]
    )
    own_hidden = pltpu.make_async_copy(picked_ref.at[here], hidden.at[:, rows_of(here)], own_sem.at[2])
    own_hidden.start()
    heads = scales_ref.shape[0]
    cosine = jnp.concatenate([cos_ref[...], cos_ref[...]], axis=1)
    sine = jnp.concatenate([sin_ref[...], -sin_ref[...]], axis=1)
    for head in range(heads):
        cols = pl.ds(head * HD, HD)
        values = grad_ref[:, cols].astype(jnp.float32)
        swapped = jnp.concatenate([values[:, HD // 2 :], values[:, : HD // 2]], axis=1)
        rot_ref[:, cols] = (values * cosine + swapped * sine).astype(jnp.bfloat16)
    for head in range(heads):
        cols = pl.ds(head * HD, HD)
        scale = jnp.broadcast_to(scales_ref[head : head + 1, :], (HD, scales_ref.shape[1])).T
        weights_ref[:, cols] = (quant_ref[:, cols].astype(jnp.float32) * scale).astype(jnp.bfloat16)
        if head == 0:
            hide(beside).start()
            own_rot.start()
            for step in range(1, group_total):
                spread(step).start()
    own_weights.start()
    for step in range(1, group_total):
        weigh(step).start()

    def hide_at(rise, across):
        level = z + rise

        @pl.when((level >= 0) & (level < depth))
        def _():
            hide(level * LINE + (1 - y if across else y)).start()

    own_rot.wait()
    for step in range(1, group_total):
        spread(step).wait_recv()

    below, above = here - LINE, here + LINE

    def travel(owner, go_up, go_down, act, piece):
        @pl.when(go_up)
        def _():
            act(relay(owner, up_send, above, piece))

        @pl.when(go_down)
        def _():
            act(relay(owner, down_send, below, piece))

    def begin(copy):
        copy.start()

    def finish(copy):
        copy.wait_send()

    def send_piece(owner, act_remote, act_local):
        source = outgoing.at[owner]

        def give(to_chunk, index, send, slot):
            mine = (owner == here) & (to_chunk == part)

            @pl.when(jnp.logical_not(mine))
            def _():
                act_remote(remote(source, pieces_out.at[index], send, o_recv.at[index], (owner, to_chunk)))

            @pl.when(mine)
            def _():
                act_local(pltpu.make_async_copy(source, pieces_out.at[index], local_sem.at[slot]))

        near = lax.rem(here, per_chunk)
        give(home, 1 + near * group_total + part, o_send.at[owner], 0)

        @pl.when((near == per_chunk - 1) & (part == group_total - 1) & (home < group_total - 1))
        def _():
            give(home + 1, 0, e_send.at[owner], 1)

        @pl.when((near == 0) & (part == 0) & (home > 0))
        def _():
            give(home - 1, last_piece, e_send.at[owner], 1)

    for piece in range(pieces):
        travel(here, z < depth - 1, z > 0, begin, piece)
        relay(here, side_send, beside, piece).start()
    hide_at(1, False)
    hide_at(-1, False)

    def produce(owner):
        outgoing[owner] = lax.dot_general(
            weights[...], rotated[rows_of(owner), :], (((1,), (1,)), ((), ())),
            preferred_element_type=jnp.float32,
        ).astype(jnp.bfloat16)

    def stage_items(away):
        items = []
        for sign in (-1, 1):
            if 0 < away < depth:
                items.append((z + sign * away, y))
            if away > 1 or (away == 1 and sign < 0):
                items.append((z + sign * (away - 1), 1 - y))
        return items

    for away in range(1, depth + 2):
        for sign in (-1, 1):
            if away < depth:
                level = z + sign * away
                owner = level * LINE + y

                @pl.when((level >= 0) & (level < depth))
                def _():
                    for piece in range(pieces):
                        relay(owner, up_send, here, piece).wait_recv()
                        if sign < 0:
                            travel(owner, z < depth - 1, z < 0, begin, piece)
                        else:
                            travel(owner, z < 0, z > 0, begin, piece)
                        relay(owner, side_send, beside, piece).start()
                        share(owner, piece).start()

            if away <= depth and (away > 1 or sign < 0):
                level_near = z + sign * (away - 1)
                other = level_near * LINE + (1 - y)

                @pl.when((level_near >= 0) & (level_near < depth))
                def _():
                    for piece in range(pieces):
                        relay(other, up_send, here, piece).wait_recv()
                        share(other, piece).start()

        if away < depth:
            hide_at(away, True)
            hide_at(-away, True)
        if away + 1 < depth:
            hide_at(away + 1, False)
            hide_at(-away - 1, False)
        if away == 2:
            own_weights.wait()
            for step in range(1, group_total):
                weigh(step).wait_recv()
            produce(here)
            send_piece(here, begin, begin)
        ready = stage_items(away - 1)
        for level, row in ready:

            @pl.when((level >= 0) & (level < depth))
            def _():
                for piece in range(pieces):
                    share(level * LINE + row, piece).wait_recv()
                produce(level * LINE + row)

        for level, row in ready:

            @pl.when((level >= 0) & (level < depth))
            def _():
                send_piece(level * LINE + row, begin, begin)

    own_hidden.wait()
    for step in range(1, owners_n):
        hidden_from(lax.rem(here + step, owners_n)).wait_recv()

    def send_grad(step):
        target = lax.rem(part + step, group_total)
        return remote(
            grad_send.at[target], grad_out.at[part], g_send.at[step - 1], g_recv.at[step - 1], (here, target)
        )

    def reduce(step, carry):
        target = lax.rem(part + step, group_total)
        grad_send[target] = jnp.dot(
            hidden[...], rotated[:, cols_of(target)], preferred_element_type=jnp.float32
        ).astype(jnp.bfloat16)

        @pl.when(step > 1)
        def _():
            send_grad(step - 1).start()

        return carry

    lax.fori_loop(1, group_total + 1, reduce, 0)
    own_grad = pltpu.make_async_copy(grad_send.at[part], grad_out.at[part], own_sem.at[3])
    own_grad.start()

    for owner in range(owners_n):
        send_piece(jnp.int32(owner), finish, lambda copy: copy.wait())
    for near in range(per_chunk):
        for source in range(group_total):
            index = 1 + near * group_total + source

            @pl.when(jnp.logical_not((home == part) & (here == part * per_chunk + near) & (part == source)))
            def _():
                remote(outgoing.at[0], pieces_out.at[index], o_send.at[0], o_recv.at[index], (here, partner)).wait_recv()

    for index, exists, mine in (
        (0, part > 0, (here == part * per_chunk - 1) & (part == group_total - 1)),
        (last_piece, part < group_total - 1, (here == (part + 1) * per_chunk) & (part == 0)),
    ):

        @pl.when(exists & jnp.logical_not(mine))
        def _():
            remote(outgoing.at[0], pieces_out.at[index], o_send.at[0], o_recv.at[index], (here, partner)).wait_recv()

    own_grad.wait()
    for step in range(1, group_total):
        send_grad(step).wait_send()
        remote(grad_send.at[0], grad_out.at[0], g_send.at[step - 1], g_recv.at[step - 1], (here, partner)).wait_recv()
    for step in range(1, group_total):
        spread(step).wait_send()
        weigh(step).wait_send()
    for step in range(1, owners_n):
        hide(lax.rem(here + step, owners_n)).wait_send()
    for piece in range(pieces):
        travel(here, z < depth - 1, z > 0, finish, piece)
        relay(here, side_send, beside, piece).wait_send()
    for away in range(1, depth):
        for sign in (-1, 1):
            level = z + sign * away
            owner = level * LINE + y

            @pl.when((level >= 0) & (level < depth))
            def _():
                for piece in range(pieces):
                    if sign < 0:
                        travel(owner, z < depth - 1, z < 0, finish, piece)
                    else:
                        travel(owner, z < 0, z > 0, finish, piece)
                    relay(owner, side_send, beside, piece).wait_send()

    def drain(step, carry):
        for piece in range(pieces):
            share(lax.rem(here + step, owners_n), piece).wait_send()
        return carry

    lax.fori_loop(1, owners_n, drain, 0)


def exchange_plan(hidden_in, key_grad, positions, key_quant, key_scales, block_counts):
    owners_n = lax.axis_size("fsdp")
    group_total = lax.axis_size("tp")
    slot_count, width = key_quant.shape
    tokens_here, row_total = hidden_in.shape
    quarter = slot_count // group_total
    chunk = row_total // group_total
    per_chunk = owners_n // group_total
    columns = width * group_total
    vmem = pl.BlockSpec(memory_space=pltpu.VMEM)
    anywhere = pl.BlockSpec(memory_space=pl.ANY)
    smem = pl.BlockSpec(memory_space=pltpu.SMEM)
    span = -(-(quarter + LANES) // LANES) * LANES
    cosine, sine = rotary_tables(positions)
    picked = pl.pallas_call(
        functools.partial(pick_kernel, owners_n, group_total, span),
        out_shape=jax.ShapeDtypeStruct((owners_n, quarter, tokens_here), jnp.bfloat16),
        in_specs=[smem, anywhere],
        out_specs=vmem,
        scratch_shapes=[
            pltpu.VMEM((owners_n, tokens_here, span), jnp.bfloat16),
            pltpu.VMEM((owners_n, 2 * span + quarter, tokens_here), jnp.float32),
            pltpu.SemaphoreType.DMA((owners_n,)),
        ],
        name="pick",
    )(block_counts, hidden_in)

    relays_n = owners_n * group_total // 2
    pieces_n = 2 + per_chunk * group_total
    dma = pltpu.SemaphoreType.DMA
    weight_grad, pieces = pl.pallas_call(
        functools.partial(exchange_kernel, owners_n, group_total),
        out_shape=(
            jax.ShapeDtypeStruct((group_total, quarter, width), jnp.bfloat16),
            jax.ShapeDtypeStruct((pieces_n, quarter, tokens_here), jnp.bfloat16),
        ),
        in_specs=[vmem] * 6,
        out_specs=(vmem,) * 2,
        scratch_shapes=[
            pltpu.VMEM((tokens_here, width), jnp.bfloat16),
            pltpu.VMEM((slot_count, width), jnp.bfloat16),
            pltpu.VMEM((owners_n * tokens_here, columns), jnp.bfloat16),
            pltpu.VMEM((quarter, columns), jnp.bfloat16),
            pltpu.VMEM((quarter, owners_n * tokens_here), jnp.bfloat16),
            pltpu.VMEM((owners_n, quarter, tokens_here), jnp.bfloat16),
            pltpu.VMEM((group_total, quarter, width), jnp.bfloat16),
            dma((4,)),
            dma((group_total - 1,)), dma((group_total - 1,)),
            dma((group_total - 1,)), dma((group_total - 1,)),
            dma((owners_n,)), dma((owners_n,)),
            dma((relays_n,)), dma((relays_n,)), dma((relays_n,)), dma((relays_n,)),
            dma((relays_n,)), dma((relays_n,)),
            dma((owners_n,)), dma((owners_n,)), dma((pieces_n,)),
            dma((group_total - 1,)), dma((group_total - 1,)),
            dma((2,)),
        ],
        compiler_params=pltpu.CompilerParams(has_side_effects=True),
        name="exchange",
    )(picked, key_grad, cosine, sine, key_quant, key_scales.T)

    margin = max(
        max(
            chunk * (owner // per_chunk) - offset_range(owner - 1, owners_n, row_total, slot_count)[0]
            for owner in range(per_chunk, owners_n, per_chunk)
        ),
        2 * quarter,
    ) if group_total > 1 else 2 * quarter
    pad = -(-(margin + slot_count) // 8) * 8
    return pl.pallas_call(
        functools.partial(assemble_kernel, owners_n, group_total, pad),
        out_shape=(
            jax.ShapeDtypeStruct((slot_count, width), jnp.bfloat16),
            jax.ShapeDtypeStruct((tokens_here, chunk), jnp.bfloat16),
        ),
        in_specs=[smem, vmem, vmem],
        out_specs=(vmem,) * 2,
        scratch_shapes=[pltpu.VMEM((chunk + 2 * pad, tokens_here), jnp.float32)],
        name="assemble",
    )(block_counts, pieces, weight_grad)


def rotary_backward(key_grad, positions):
    tokens_here = key_grad.shape[0]
    half_dim = HD // 2
    cotangent = key_grad.astype(jnp.float32).reshape(tokens_here, -1, HD)
    freq_idx = jnp.arange(half_dim, dtype=jnp.float32)
    inverse = jnp.exp(-(2.0 * freq_idx / HD) * math.log(rope_base))
    angles = positions.astype(jnp.float32)[:, None] * inverse[None, :]
    cosine = jnp.cos(angles)[:, None, :]
    sine_part = jnp.sin(angles)[:, None, :]
    lower_half = cotangent[..., :half_dim]
    upper_half = cotangent[..., half_dim:]
    back_lower = lower_half * cosine + upper_half * sine_part
    back_upper = upper_half * cosine - lower_half * sine_part
    joined = jnp.concatenate([back_lower, back_upper], axis=-1)
    return joined.reshape(tokens_here, -1).astype(jnp.bfloat16)


def slot_tables(block_counts, slot_count, row_total):
    offsets = jnp.cumsum(block_counts) - block_counts
    owners_n = block_counts.shape[0]
    slot_ids = jnp.arange(owners_n * slot_count, dtype=jnp.int32)
    within = slot_ids % slot_count
    live_counts = jnp.broadcast_to(block_counts[:, None], (owners_n, slot_count)).reshape(-1)
    base_rows = jnp.broadcast_to(offsets[:, None], (owners_n, slot_count)).reshape(-1)
    is_live = within < live_counts
    row_of_slot = jnp.where(is_live, base_rows + within, 0)
    row_ids = jnp.arange(row_total, dtype=jnp.int32)
    at_or_after = row_ids[:, None] >= offsets[None, :]
    owner_of_row = jnp.sum(at_or_after.astype(jnp.int32), axis=1) - 1
    row_begin = jnp.max(jnp.where(at_or_after, offsets[None, :], 0), axis=1)
    slot_of_row = owner_of_row * slot_count + row_ids - row_begin
    return (row_of_slot, is_live, slot_of_row)


def gather_plan(hidden_in, key_grad, positions, key_quant, key_scales, block_counts):
    slot_count = key_quant.shape[0]
    local_heads = key_scales.shape[1]
    row_total = hidden_in.shape[1]
    row_of_slot, is_live, slot_of_row = slot_tables(block_counts, slot_count, row_total)
    scaled = (
        key_quant.astype(jnp.float32).reshape(slot_count, local_heads, HD) * key_scales[:, :, None]
    )
    local_weights = scaled.astype(jnp.bfloat16).reshape(slot_count, local_heads * HD)
    rotated = rotary_backward(key_grad, positions)
    picked = jnp.where(
        is_live[None, :], jnp.take(hidden_in, row_of_slot, axis=1), jnp.zeros((), jnp.bfloat16)
    )
    weight_grad = lax.psum_scatter(
        lax.dot_general(
            picked, rotated, (((0,), (0,)), ((), ())), preferred_element_type=jnp.float32
        ),
        "fsdp",
        scatter_dimension=0,
        tiled=True,
    ).astype(jnp.bfloat16)
    group_total = lax.axis_size("tp")
    whole_slots = lax.all_gather(local_weights, "fsdp", axis=0, tiled=True)
    ordered = jnp.take(whole_slots, slot_of_row, axis=0)
    own_rows = lax.all_to_all(ordered, "tp", split_axis=0, concat_axis=1, tiled=True)
    all_heads = lax.all_gather(rotated, "tp", axis=1, tiled=True)
    tokens_here = all_heads.shape[0]
    feature_here = own_rows.shape[0]
    heads_grouped = all_heads.reshape(tokens_here, group_total, -1)
    rows_grouped = own_rows.reshape(feature_here, group_total, -1)
    group_part = jnp.einsum(
        "tgk,dgk->gtd", heads_grouped, rows_grouped, preferred_element_type=jnp.float32
    ).astype(jnp.bfloat16)
    input_grad = jnp.sum(group_part.astype(jnp.float32), axis=0).astype(jnp.bfloat16)
    return (weight_grad, input_grad)


def per_device(hidden_in, key_grad, positions, key_quant, key_scales, block_counts):
    tokens_here, row_total = hidden_in.shape
    slot_count, width = key_quant.shape
    fits = exchange_fits(
        lax.axis_size("fsdp"), lax.axis_size("tp"), slot_count, row_total, tokens_here, width
    )
    plan = exchange_plan if fits else gather_plan
    return plan(hidden_in, key_grad, positions, key_quant, key_scales, block_counts)


def solution(mesh):
    in_specs = (P("fsdp", None), P("fsdp", "tp"), P("fsdp"), P("fsdp", "tp"), P("fsdp", "tp"), P())
    out_specs = (P("fsdp", "tp"), P("fsdp", "tp"))
    return jax.shard_map(
        per_device, mesh=mesh, in_specs=in_specs, out_specs=out_specs, check_vma=False
    )
```
